32 devices in a mesh: row: 4 (over z), col: 8 (over y, x, core).
Axes of the slice: x: 2, y: 2, z: 4, core: 2. Of those that a mesh axis runs over, the one named last changes fastest.
Arguments:
- rho_real: float32 [4096, 4096], P('row', 'col'), may hold values from -2.5 to 4, as said below
- rho_imag: float32 [4096, 4096], P('row', 'col'), may hold values from -2.5 to 2.5, as said below
- hamiltonian: bfloat16 [4096, 4096], P('row', 'col'), may hold values from -1 to 1
- amplitudes: float32 [8, 4096], replicated, may hold values from 0.15 to 0.6
- offsets: int32 [8], replicated, may hold values from -16 to 16
- active_jumps: int32 [1], replicated, may hold values from 4 to 8
Outputs:
- rho_next_real: float32 [4096, 4096], P('row', 'col')
- rho_next_imag: float32 [4096, 4096], P('row', 'col')
The draws below stay inside these ranges and needn't reach their ends.
Inputs may be any that keep to these rules, and one draw needn't show every extreme that they name: `rho_real`: symmetric, with every diagonal entry 0.5 or more. `rho_imag`: antisymmetric.
All inputs are finite; a program needn't handle non-finite values.
Results may differ from the reference program's by a relative error of at most 0.001.
Values may be sent and summed in bfloat16 or wider, within the bound.
A program may use at most 192 MiB of HBM per device.

```python
import math
import jax
import jax.numpy as jnp
from jax import lax

N = 4096
K = 8
OMAX = 16


def fluctuation(key):
    return jnp.clip(jax.random.normal(key, (N, N), jnp.float32), -3.0, 3.0)


def draw_rho_real(key, part):
    values = fluctuation(jax.random.fold_in(key, 11))
    spread = (values + values.T) * 0.35
    diagonal = jax.random.uniform(jax.random.fold_in(key, 12), (N,), jnp.float32, 0.5, 2.0)
    row_index = lax.broadcasted_iota(jnp.int32, (N, N), 0)
    col_index = lax.broadcasted_iota(jnp.int32, (N, N), 1)
    return jnp.where(row_index == col_index, diagonal[:, None], spread)


def draw_rho_imag(key, part):
    values = fluctuation(jax.random.fold_in(key, 21))
    return (values - values.T) * 0.35


def draw_hamiltonian(key, part):
    values = fluctuation(jax.random.fold_in(key, 31))
    return ((values + values.T) * (0.7 / math.sqrt(N))).astype(jnp.bfloat16)


def plant(drawn, own_key, low, high):
    longest = drawn.shape.index(max(drawn.shape))
    spots = []
    for shift in (0, 1):
        where = [jax.random.randint(jax.random.fold_in(own_key, axis), (), 0, length) for axis, length in enumerate(drawn.shape)]
        where[longest] = (where[longest] + shift) % drawn.shape[longest]
        spots.append(tuple(where))
    return drawn.at[spots[0]].set(low).at[spots[1]].set(high)


def setup_inputs(seed: int = 0) -> dict:
    keys = jax.random.split(jax.random.key(seed), 7)
    rho_real = draw_rho_real(jax.random.fold_in(keys[6], 71), 0)
    rho_imag = draw_rho_imag(jax.random.fold_in(keys[6], 71), 0)
    hamiltonian = draw_hamiltonian(jax.random.fold_in(keys[6], 71), 0)
    amplitudes = jnp.clip(jnp.exp(jax.random.uniform(keys[3], (K, N), jnp.float32, math.log(0.15), math.log(0.6))), 0.15, 0.6)
    offsets = plant(jax.random.randint(keys[4], (K,), -OMAX, OMAX + 1), jax.random.fold_in(keys[4], 1), -OMAX, OMAX).astype(jnp.int32)
    active_jumps = jax.random.randint(keys[5], (1,), K // 2, K + 1).astype(jnp.int32)
    return dict(rho_real=rho_real, rho_imag=rho_imag, hamiltonian=hamiltonian, amplitudes=amplitudes, offsets=offsets, active_jumps=active_jumps)


step_size = 0.25


def dissipate(matrix, padded, amplitudes, offsets, active, row_first, col_first):
    height = matrix.shape[1]
    breadth = matrix.shape[2]
    levels = amplitudes.shape[1]
    margin = (padded.shape[1] - height) // 2
    positions = jnp.arange(levels, dtype=jnp.int32)
    summed = jnp.zeros(matrix.shape, matrix.dtype)
    for jump_slot in range(amplitudes.shape[0]):
        offset = offsets[jump_slot].astype(jnp.int32)
        inside = (positions + offset >= 0) & (positions + offset < levels)
        strength = jnp.where(inside, amplitudes[jump_slot], 0.0)
        outflow = jnp.pad(strength * strength, (margin, margin))
        outflow = lax.dynamic_slice_in_dim(outflow, (margin - offset).astype(jnp.int32), levels)
        row_strength = lax.dynamic_slice_in_dim(strength, row_first, height)
        col_strength = lax.dynamic_slice_in_dim(strength, col_first, breadth)
        row_outflow = lax.dynamic_slice_in_dim(outflow, row_first, height)
        col_outflow = lax.dynamic_slice_in_dim(outflow, col_first, breadth)
        corner = (margin + offset).astype(jnp.int32)
        shifted = lax.dynamic_slice(padded, (jnp.int32(0), corner, corner), (2, height, breadth))
        contribution = (row_strength[:, None] * col_strength[None, :]) * shifted - 0.5 * (row_outflow[:, None] + col_outflow[None, :]) * matrix
        summed = summed + jnp.where(jump_slot < active, contribution, 0.0)
    return summed


def drift(real_part, imag_part, hamiltonian, amplitudes, offsets, active):
    real_low = real_part.astype(jnp.bfloat16)
    imag_low = imag_part.astype(jnp.bfloat16)
    left_real = jnp.dot(hamiltonian, real_low, preferred_element_type=jnp.float32)
    right_real = jnp.dot(real_low, hamiltonian, preferred_element_type=jnp.float32)
    left_imag = jnp.dot(hamiltonian, imag_low, preferred_element_type=jnp.float32)
    right_imag = jnp.dot(imag_low, hamiltonian, preferred_element_type=jnp.float32)
    matrix = jnp.stack([real_part, imag_part])
    padded = jnp.pad(matrix, ((0, 0), (OMAX, OMAX), (OMAX, OMAX)))
    loss = dissipate(matrix, padded, amplitudes, offsets, active, jnp.int32(0), jnp.int32(0))
    return left_imag - right_imag + loss[0], right_real - left_real + loss[1]


def reference(rho_real, rho_imag, hamiltonian, amplitudes, offsets, active_jumps):
    active = active_jumps[0]
    first_real, first_imag = drift(rho_real, rho_imag, hamiltonian, amplitudes, offsets, active)
    middle_real = rho_real + step_size * first_real
    middle_imag = rho_imag + step_size * first_imag
    middle_trace = jnp.trace(middle_real)
    rescale = N / middle_trace
    middle_real = middle_real * rescale
    middle_imag = middle_imag * rescale
    second_real, second_imag = drift(middle_real, middle_imag, hamiltonian, amplitudes, offsets, active)
    updated_real = rho_real + 0.5 * step_size * (first_real + second_real)
    updated_imag = rho_imag + 0.5 * step_size * (first_imag + second_imag)
    final_trace = jnp.trace(updated_real)
    rescale = N / final_trace
    return updated_real * rescale, updated_imag * rescale
```

```python
import functools

import jax
import jax.numpy as jnp
from jax import lax
from jax.experimental import pallas as pl
from jax.experimental.pallas import tpu as pltpu
from jax.sharding import PartitionSpec as P

OMAX = 16


step_size = 0.25

VMEM_LIMIT = 62 * 1024 * 1024


def ring_plan(count, favour_up):
    far = count // 2
    near = count - 1 - far
    return (far, near) if favour_up else (near, far)


def top(mask):
    return mask.bit_length() - 1


def commutator_kernel(first, nz, nc, *refs):
    if first:
        (real, imag, ham, out_real, out_imag, ham_rows_out, ham_cols_out,
         ham_rows, ham_cols, real_rows, imag_rows, real_cols, imag_cols,
         xy_send, xy_recv, z_send, z_recv, local_sem) = refs
    else:
        (real, imag, ham_rows_in, ham_cols_in, out_real, out_imag,
         ham_rows, ham_cols, real_rows, imag_rows, real_cols, imag_cols,
         xy_send, xy_recv, z_send, z_recv, local_sem) = refs
        ham = None
    height, breadth = real.shape
    z = lax.axis_index("row")
    c = lax.axis_index("col")
    bits = nc.bit_length() - 1
    half = height // 2
    physical = list(range(1, bits))
    order_a = physical + [0]
    order_b = physical[::-1] + [0]

    pieces = []
    if first:
        pieces.append((ham, ham_rows, (0, half), order_a))
        pieces.append((ham, ham_rows, (half, half), order_b))
    pieces.append((real, real_rows, (0, height), order_a))
    pieces.append((imag, imag_rows, (0, height), order_b))
    rings = []
    if first:
        rings.append((ham, ham_cols, (0, half), True))
        rings.append((ham, ham_cols, (half, half), False))
    rings.append((real, real_cols, (0, height), True))
    rings.append((imag, imag_cols, (0, height), False))

    barrier = pltpu.get_barrier_semaphore()
    up = lax.rem(z + 1, nz)
    down = lax.rem(z + nz - 1, nz)

    def flip(index, b):
        weight = 1 << b
        bit = lax.rem(index // weight, 2)
        return index + weight * (1 - 2 * bit)

    def masked(mask, order):
        index = c
        for t in range(bits):
            if mask >> t & 1:
                index = flip(index, order[t])
        return index

    for neighbour in (up, down):
        pl.semaphore_signal(barrier, inc=1, device_id=(neighbour, c), device_id_type=pl.DeviceIdType.MESH)
    for b in range(bits):
        pl.semaphore_signal(barrier, inc=1, device_id=(z, flip(c, b)), device_id_type=pl.DeviceIdType.MESH)
    pl.semaphore_wait(barrier, 2 + bits)

    def xy_copy(p, mask, t):
        own, panel, (start, size), order = pieces[p]
        index = masked(mask, order)
        rows = pl.ds(start, size)
        source = own.at[rows, :] if mask == 0 else panel.at[index, rows, :]
        arrival = mask | 1 << t
        return pltpu.make_async_remote_copy(
            src_ref=source,
            dst_ref=panel.at[index, rows, :],
            send_sem=xy_send.at[p, arrival],
            recv_sem=xy_recv.at[p, arrival],
            device_id=(z, flip(c, order[t])),
            device_id_type=pl.DeviceIdType.MESH,
        )

    def z_copy(p, direction, step):
        own, panel, (start, size), _ = rings[p]
        rows = pl.ds(start, size)
        shift = nz - (step - 1) if direction == 0 else step - 1
        index = lax.rem(z + shift, nz)
        source = own.at[rows, :] if step == 1 else panel.at[index, rows, :]
        return pltpu.make_async_remote_copy(
            src_ref=source,
            dst_ref=panel.at[index, rows, :],
            send_sem=z_send.at[p, direction, step],
            recv_sem=z_recv.at[p, direction, step],
            device_id=(up if direction == 0 else down, c),
            device_id_type=pl.DeviceIdType.MESH,
        )

    started = []

    def begin(copy):
        copy.start()
        started.append(copy)

    for p in range(len(pieces)):
        for t in range(bits):
            begin(xy_copy(p, 0, t))
    for p in range(len(rings)):
        plan = ring_plan(nz, rings[p][3])
        for direction in (0, 1):
            if plan[direction] >= 1:
                begin(z_copy(p, direction, 1))

    if first:
        locals_in = [
            pltpu.make_async_copy(ham, ham_rows.at[c], local_sem.at[0]),
            pltpu.make_async_copy(ham, ham_cols.at[z], local_sem.at[1]),
        ]
    else:
        locals_in = [
            pltpu.make_async_copy(ham_rows_in, ham_rows, local_sem.at[0]),
            pltpu.make_async_copy(ham_cols_in, ham_cols, local_sem.at[1]),
        ]
    for copy in locals_in:
        copy.start()

    def advance_xy(p, mask):
        order_t = top(mask)
        xy_copy(p, mask & ~(1 << order_t), order_t).wait_recv()
        for t in range(order_t + 1, bits):
            begin(xy_copy(p, mask, t))

    def advance_z(p, direction, step):
        plan = ring_plan(nz, rings[p][3])
        z_copy(p, direction, step).wait_recv()
        if step < plan[direction]:
            begin(z_copy(p, direction, step + 1))

    ring_steps = max(ring_plan(nz, True))

    def ring_events(p, step):
        plan = ring_plan(nz, rings[p][3])
        return [(p, d, step) for d in (0, 1) if step <= plan[d]]

    base = 0
    if first:
        base = 2
        for mask in range(1, nc):
            for p in (0, 1):
                advance_xy(p, mask)
            if mask <= ring_steps:
                for p in (0, 1):
                    for event in ring_events(p, mask):
                        advance_z(*event)
        for step in range(nc, ring_steps + 1):
            for p in (0, 1):
                for event in ring_events(p, step):
                    advance_z(*event)
    for copy in locals_in:
        copy.wait()
    outs = []
    if first:
        outs = [
            pltpu.make_async_copy(ham_rows, ham_rows_out, local_sem.at[0]),
            pltpu.make_async_copy(ham_cols, ham_cols_out, local_sem.at[1]),
        ]
        for copy in outs:
            copy.start()

    per = height // breadth
    tile = min(256, height)

    def rows_product(out, block, index, sign, fresh):
        k = index // per
        offset = pl.multiple_of(lax.rem(index, per) * breadth, breadth)

        @pl.loop(0, height // tile)
        def _(i):
            here = pl.ds(pl.multiple_of(i * tile, tile), tile)
            product = jnp.dot(
                block[here, :], ham_cols[k, pl.ds(offset, breadth), :], preferred_element_type=jnp.float32
            )
            if fresh:
                out[here, :] = product if sign > 0 else -product
            elif sign > 0:
                out[here, :] += product
            else:
                out[here, :] -= product

    def cols_product(out, block, k, sign):
        @pl.loop(0, height // tile)
        def _(i):
            here = pl.ds(pl.multiple_of(i * tile, tile), tile)
            product = jnp.dot(
                ham_rows[k * per, here, :], block[pl.ds(0, breadth), :], preferred_element_type=jnp.float32
            )
            for part in range(1, per):
                product += jnp.dot(
                    ham_rows[k * per + part, here, :],
                    block[pl.ds(part * breadth, breadth), :],
                    preferred_element_type=jnp.float32,
                )
            if sign > 0:
                out[here, :] += product
            else:
                out[here, :] -= product

    rows_product(out_imag, real, c, 1, True)
    rows_product(out_real, imag, c, -1, True)
    cols_product(out_imag, real, z, -1)
    cols_product(out_real, imag, z, 1)
    sides = ((real_rows, real_cols, out_imag, 1), (imag_rows, imag_cols, out_real, -1))

    def consume_ring(step):
        for side, (_, cols, out, sign) in enumerate(sides):
            for p, direction, s in ring_events(base + side, step):
                advance_z(p, direction, s)
                shift = nz - s if direction == 0 else s
                k = lax.rem(z + shift, nz)
                cols_product(out, cols.at[k], k, -sign)

    done_steps = 0
    for mask in range(1, nc):
        for side, (rows, _, out, sign) in enumerate(sides):
            p = base + side
            advance_xy(p, mask)
        for side, (rows, _, out, sign) in enumerate(sides):
            index = masked(mask, pieces[base + side][3])
            rows_product(out, rows.at[index], index, sign, False)
        want = mask * ring_steps // (nc - 1) if nc > 1 else ring_steps
        while done_steps < want:
            done_steps += 1
            consume_ring(done_steps)
    for copy in started:
        copy.wait_send()
    for copy in outs:
        copy.wait()


def commutator(real_low, imag_low, ham, panels, nz, nc):
    height, breadth = real_low.shape
    first = panels is None
    vmem = pl.BlockSpec(memory_space=pltpu.VMEM)
    anywhere = pl.BlockSpec(memory_space=pl.ANY)
    drift_shape = jax.ShapeDtypeStruct((height, breadth), jnp.float32)
    low = jnp.bfloat16
    rows_shape = (nc, height, breadth)
    cols_shape = (nz, height, breadth)
    out_shape = [drift_shape, drift_shape]
    out_specs = [vmem, vmem]
    if first:
        out_shape += [jax.ShapeDtypeStruct(rows_shape, low), jax.ShapeDtypeStruct(cols_shape, low)]
        out_specs += [anywhere, anywhere]
        in_specs = [vmem] * 3
        operands = (real_low, imag_low, ham)
    else:
        in_specs = [vmem, vmem, anywhere, anywhere]
        operands = (real_low, imag_low) + tuple(panels)
    count = 4 if first else 2
    flops = 8 * height * breadth * nz * height
    return pl.pallas_call(
        functools.partial(commutator_kernel, first, nz, nc),
        out_shape=out_shape,
        in_specs=in_specs,
        out_specs=out_specs,
        scratch_shapes=[
            pltpu.VMEM(rows_shape, low),
            pltpu.VMEM(cols_shape, low),
            pltpu.VMEM(rows_shape, low),
            pltpu.VMEM(rows_shape, low),
            pltpu.VMEM(cols_shape, low),
            pltpu.VMEM(cols_shape, low),
            pltpu.SemaphoreType.DMA((count, nc)),
            pltpu.SemaphoreType.DMA((count, nc)),
            pltpu.SemaphoreType.DMA((count, 2, nz)),
            pltpu.SemaphoreType.DMA((count, 2, nz)),
            pltpu.SemaphoreType.DMA((2,)),
        ],
        compiler_params=pltpu.CompilerParams(
            collective_id=0 if first else 1, has_side_effects=True, vmem_limit_bytes=VMEM_LIMIT
        ),
        cost_estimate=pl.CostEstimate(flops=flops, bytes_accessed=16 * height * breadth, transcendentals=0),
        name="first_commutator" if first else "second_commutator",
    )(*operands)


def extended(cells, sides, width):
    for axis, dim in sides:
        count = lax.axis_size(axis)
        ends = count - 1
        head = lax.slice_in_dim(cells, 0, width, axis=dim)
        tail = lax.slice_in_dim(cells, cells.shape[dim] - width, cells.shape[dim], axis=dim)
        cells = jnp.concatenate(
            [
                lax.ppermute(tail, axis, [(i, (i + 1) % count) for i in range(ends)]),
                cells,
                lax.ppermute(head, axis, [((i + 1) % count, i) for i in range(ends)]),
            ],
            axis=dim,
        )
    return cells


def dissipate(matrix, padded, amplitudes, offsets, active, row_first, col_first):
    height = matrix.shape[1]
    breadth = matrix.shape[2]
    levels = amplitudes.shape[1]
    margin = (padded.shape[1] - height) // 2
    positions = jnp.arange(levels, dtype=jnp.int32)
    summed = jnp.zeros(matrix.shape, matrix.dtype)
    for jump_slot in range(amplitudes.shape[0]):
        offset = offsets[jump_slot]
        inside = (positions + offset >= 0) & (positions + offset < levels)
        strength = jnp.where(inside, amplitudes[jump_slot], 0.0)
        outflow = jnp.pad(strength * strength, (margin, margin))
        outflow = lax.dynamic_slice_in_dim(outflow, margin - offset, levels)
        row_strength = lax.dynamic_slice_in_dim(strength, row_first, height)
        col_strength = lax.dynamic_slice_in_dim(strength, col_first, breadth)
        row_outflow = lax.dynamic_slice_in_dim(outflow, row_first, height)
        col_outflow = lax.dynamic_slice_in_dim(outflow, col_first, breadth)
        corner = margin + offset
        shifted = lax.dynamic_slice(padded, (jnp.int32(0), corner, corner), (2, height, breadth))
        contribution = (
            row_strength[:, None] * col_strength[None, :] * shifted
            - 0.5 * (row_outflow[:, None] + col_outflow[None, :]) * matrix
        )
        summed = summed + jnp.where(jump_slot < active, contribution, 0.0)
    return summed


def diagonal_sum(matrix, row_first, col_first):
    row_index = lax.broadcasted_iota(jnp.int32, matrix.shape, 0) + row_first
    col_index = lax.broadcasted_iota(jnp.int32, matrix.shape, 1) + col_first
    return jnp.sum(jnp.where(row_index == col_index, matrix, 0.0))


def local(nz, nc, rho_real, rho_imag, hamiltonian, amplitudes, offsets, active_jumps):
    height, breadth = rho_real.shape
    levels = amplitudes.shape[1]
    row_first = lax.axis_index("row") * height
    col_first = lax.axis_index("col") * breadth
    active = active_jumps[0]
    start_trace = lax.psum(diagonal_sum(rho_real, row_first, col_first), ("row", "col"))

    def drift(real_part, imag_part, panels):
        real_low = real_part.astype(jnp.bfloat16)
        imag_low = imag_part.astype(jnp.bfloat16)
        real_turn, imag_turn, *made = commutator(real_low, imag_low, hamiltonian, panels, nz, nc)
        matrix = jnp.stack([real_part, imag_part])
        padded = extended(matrix.astype(jnp.bfloat16), (("row", 1), ("col", 2)), OMAX).astype(
            matrix.dtype
        )
        loss = dissipate(matrix, padded, amplitudes, offsets, active, row_first, col_first)
        return real_turn + loss[0], imag_turn + loss[1], made

    first_real, first_imag, panels = drift(rho_real, rho_imag, None)
    rescale = levels / start_trace
    middle_real = (rho_real + step_size * first_real) * rescale
    middle_imag = (rho_imag + step_size * first_imag) * rescale
    second_real, second_imag, _ = drift(middle_real, middle_imag, panels)
    updated_real = rho_real + 0.5 * step_size * (first_real + second_real)
    updated_imag = rho_imag + 0.5 * step_size * (first_imag + second_imag)
    return (updated_real * rescale, updated_imag * rescale)


def solution(mesh):
    in_specs = (P("row", "col"), P("row", "col"), P("row", "col"), P(), P(), P())
    out_specs = (P("row", "col"), P("row", "col"))
    body = functools.partial(local, mesh.shape["row"], mesh.shape["col"])
    return jax.shard_map(body, mesh=mesh, in_specs=in_specs, out_specs=out_specs, check_vma=False)
```

```python
import functools

import jax
import jax.numpy as jnp
from jax import lax
from jax.experimental import pallas as pl
from jax.experimental.pallas import tpu as pltpu
from jax.sharding import PartitionSpec as P

OMAX = 16
LANES = 128


step_size = 0.25

VMEM_LIMIT = 62 * 1024 * 1024


def ring_plan(count, favour_up):
    far = count // 2
    near = count - 1 - far
    return (far, near) if favour_up else (near, far)


def top(mask):
    return mask.bit_length() - 1


def commutator_kernel(first, nz, nc, *refs):
    if first:
        (real, imag, ham, out_real, out_imag, real_wide, imag_wide, ham_rows_out, ham_cols_out,
         ham_rows, ham_cols, real_rows, imag_rows, real_cols, imag_cols, corners,
         xy_send, xy_recv, z_send, z_recv, corner_send, corner_recv, local_sem) = refs
    else:
        (real, imag, ham_rows_in, ham_cols_in, out_real, out_imag, real_wide, imag_wide,
         ham_rows, ham_cols, real_rows, imag_rows, real_cols, imag_cols, corners,
         xy_send, xy_recv, z_send, z_recv, corner_send, corner_recv, local_sem) = refs
        ham = None
    height, breadth = real.shape
    z = lax.axis_index("row")
    c = lax.axis_index("col")
    bits = nc.bit_length() - 1
    half = height // 2
    physical = list(range(1, bits))
    order_a = physical + [0]
    order_b = physical[::-1] + [0]

    pieces = []
    if first:
        pieces.append((ham, ham_rows, (0, half), order_a))
        pieces.append((ham, ham_rows, (half, half), order_b))
    pieces.append((real, real_rows, (0, height), order_a))
    pieces.append((imag, imag_rows, (0, height), order_b))
    rings = []
    if first:
        rings.append((ham, ham_cols, (0, half), True))
        rings.append((ham, ham_cols, (half, half), False))
    rings.append((real, real_cols, (0, height), True))
    rings.append((imag, imag_cols, (0, height), False))

    barrier = pltpu.get_barrier_semaphore()
    up = lax.rem(z + 1, nz)
    down = lax.rem(z + nz - 1, nz)

    def flip(index, b):
        weight = 1 << b
        bit = lax.rem(index // weight, 2)
        return index + weight * (1 - 2 * bit)

    def masked(mask, order):
        index = c
        for t in range(bits):
            if mask >> t & 1:
                index = flip(index, order[t])
        return index

    for neighbour in (up, down):
        pl.semaphore_signal(barrier, inc=1, device_id=(neighbour, c), device_id_type=pl.DeviceIdType.MESH)
    for b in range(bits):
        pl.semaphore_signal(barrier, inc=1, device_id=(z, flip(c, b)), device_id_type=pl.DeviceIdType.MESH)
    left = lax.rem(c + nc - 1, nc)
    right = lax.rem(c + 1, nc)
    diagonals = [(v, h) for v in (0, 1) for h in (0, 1)]

    def diagonal(v, h):
        return ((up, down)[v], (right, left)[h])

    for v, h in diagonals:
        pl.semaphore_signal(barrier, inc=1, device_id=diagonal(v, h), device_id_type=pl.DeviceIdType.MESH)
    pl.semaphore_wait(barrier, 2 + bits + 4)

    def corner_copy(side, v, h):
        own = (real, imag)[side]
        rows = pl.ds(height - OMAX if v == 0 else 0, OMAX)
        cols = pl.ds(breadth - LANES if h == 0 else 0, LANES)
        slot = side * 4 + v * 2 + h
        return pltpu.make_async_remote_copy(
            src_ref=own.at[rows, cols],
            dst_ref=corners.at[slot],
            send_sem=corner_send.at[slot],
            recv_sem=corner_recv.at[slot],
            device_id=diagonal(v, h),
            device_id_type=pl.DeviceIdType.MESH,
        )

    def xy_copy(p, mask, t):
        own, panel, (start, size), order = pieces[p]
        index = masked(mask, order)
        rows = pl.ds(start, size)
        source = own.at[rows, :] if mask == 0 else panel.at[index, rows, :]
        arrival = mask | 1 << t
        return pltpu.make_async_remote_copy(
            src_ref=source,
            dst_ref=panel.at[index, rows, :],
            send_sem=xy_send.at[p, arrival],
            recv_sem=xy_recv.at[p, arrival],
            device_id=(z, flip(c, order[t])),
            device_id_type=pl.DeviceIdType.MESH,
        )

    def z_copy(p, direction, step):
        own, panel, (start, size), _ = rings[p]
        rows = pl.ds(start, size)
        shift = nz - (step - 1) if direction == 0 else step - 1
        index = lax.rem(z + shift, nz)
        source = own.at[rows, :] if step == 1 else panel.at[index, rows, :]
        return pltpu.make_async_remote_copy(
            src_ref=source,
            dst_ref=panel.at[index, rows, :],
            send_sem=z_send.at[p, direction, step],
            recv_sem=z_recv.at[p, direction, step],
            device_id=(up if direction == 0 else down, c),
            device_id_type=pl.DeviceIdType.MESH,
        )

    started = []

    def begin(copy):
        copy.start()
        started.append(copy)

    def begin_own(which):
        for p in which:
            for t in range(bits):
                begin(xy_copy(p, 0, t))
            plan = ring_plan(nz, rings[p][3])
            for direction in (0, 1):
                if plan[direction] >= 1:
                    begin(z_copy(p, direction, 1))

    for side in (0, 1):
        for v, h in diagonals:
            begin(corner_copy(side, v, h))
    begin_own((0, 1))

    if first:
        locals_in = [
            pltpu.make_async_copy(ham, ham_rows.at[c], local_sem.at[0]),
            pltpu.make_async_copy(ham, ham_cols.at[z], local_sem.at[1]),
        ]
    else:
        locals_in = [
            pltpu.make_async_copy(ham_rows_in, ham_rows, local_sem.at[0]),
            pltpu.make_async_copy(ham_cols_in, ham_cols, local_sem.at[1]),
        ]
    for copy in locals_in:
        copy.start()

    def advance_xy(p, mask):
        order_t = top(mask)
        xy_copy(p, mask & ~(1 << order_t), order_t).wait_recv()
        for t in range(order_t + 1, bits):
            begin(xy_copy(p, mask, t))

    def advance_z(p, direction, step):
        plan = ring_plan(nz, rings[p][3])
        z_copy(p, direction, step).wait_recv()
        if step < plan[direction]:
            begin(z_copy(p, direction, step + 1))

    ring_steps = max(ring_plan(nz, True))

    def ring_events(p, step):
        plan = ring_plan(nz, rings[p][3])
        return [(p, d, step) for d in (0, 1) if step <= plan[d]]

    base = 0
    if first:
        base = 2
        for mask in range(1, nc):
            for p in (0, 1):
                advance_xy(p, mask)
            if mask <= ring_steps:
                for p in (0, 1):
                    for event in ring_events(p, mask):
                        advance_z(*event)
            if mask == 1:
                begin_own((2, 3))
        for step in range(nc, ring_steps + 1):
            for p in (0, 1):
                for event in ring_events(p, step):
                    advance_z(*event)
    for copy in locals_in:
        copy.wait()
    outs = []
    if first:
        outs = [
            pltpu.make_async_copy(ham_rows, ham_rows_out, local_sem.at[0]),
            pltpu.make_async_copy(ham_cols, ham_cols_out, local_sem.at[1]),
        ]
        for copy in outs:
            copy.start()

    per = height // breadth
    tile = min(256, height)

    def rows_product(out, block, index, sign, fresh):
        k = index // per
        offset = pl.multiple_of(lax.rem(index, per) * breadth, breadth)

        @pl.loop(0, height // tile)
        def _(i):
            here = pl.ds(pl.multiple_of(i * tile, tile), tile)
            product = jnp.dot(
                block[here, :], ham_cols[k, pl.ds(offset, breadth), :], preferred_element_type=jnp.float32
            )
            if fresh:
                out[here, :] = product if sign > 0 else -product
            elif sign > 0:
                out[here, :] += product
            else:
                out[here, :] -= product

    def cols_product(out, block, k, sign):
        @pl.loop(0, height // tile)
        def _(i):
            here = pl.ds(pl.multiple_of(i * tile, tile), tile)
            product = jnp.dot(
                ham_rows[k * per, here, :], block[pl.ds(0, breadth), :], preferred_element_type=jnp.float32
            )
            for part in range(1, per):
                product += jnp.dot(
                    ham_rows[k * per + part, here, :],
                    block[pl.ds(part * breadth, breadth), :],
                    preferred_element_type=jnp.float32,
                )
            if sign > 0:
                out[here, :] += product
            else:
                out[here, :] -= product

    rows_product(out_imag, real, c, 1, True)
    rows_product(out_real, imag, c, -1, True)
    cols_product(out_imag, real, z, -1)
    cols_product(out_real, imag, z, 1)
    sides = ((real_rows, real_cols, out_imag, 1), (imag_rows, imag_cols, out_real, -1))

    def consume_ring(step):
        for side, (_, cols, out, sign) in enumerate(sides):
            for p, direction, s in ring_events(base + side, step):
                advance_z(p, direction, s)
                shift = nz - s if direction == 0 else s
                k = lax.rem(z + shift, nz)
                cols_product(out, cols.at[k], k, -sign)

    done_steps = 0
    for mask in range(1, nc):
        for side, (rows, _, out, sign) in enumerate(sides):
            p = base + side
            advance_xy(p, mask)
        for side, (rows, _, out, sign) in enumerate(sides):
            index = masked(mask, pieces[base + side][3])
            rows_product(out, rows.at[index], index, sign, False)
        want = mask * ring_steps // (nc - 1) if nc > 1 else ring_steps
        while done_steps < want:
            done_steps += 1
            consume_ring(done_steps)
    for side, (rows, cols, wide) in enumerate(((real_rows, real_cols, real_wide), (imag_rows, imag_cols, imag_wide))):
        own = (real, imag)[side]
        for v, h in diagonals:
            corner_copy(side, v, h).wait_recv()
        middle = pl.ds(OMAX, height)
        inner = pl.ds(LANES, breadth)
        above, below = pl.ds(0, OMAX), pl.ds(OMAX + height, OMAX)
        before, after = pl.ds(0, LANES), pl.ds(LANES + breadth, LANES)
        wide[middle, inner] = own[...]
        wide[above, inner] = cols[down, pl.ds(height - OMAX, OMAX), :]
        wide[below, inner] = cols[up, pl.ds(0, OMAX), :]
        wide[middle, before] = rows[left, :, pl.ds(breadth - LANES, LANES)]
        wide[middle, after] = rows[right, :, pl.ds(0, LANES)]
        wide[above, before] = corners[side * 4]
        wide[above, after] = corners[side * 4 + 1]
        wide[below, before] = corners[side * 4 + 2]
        wide[below, after] = corners[side * 4 + 3]
    for copy in started:
        copy.wait_send()
    for copy in outs:
        copy.wait()


def commutator(real_low, imag_low, ham, panels, nz, nc):
    height, breadth = real_low.shape
    first = panels is None
    vmem = pl.BlockSpec(memory_space=pltpu.VMEM)
    anywhere = pl.BlockSpec(memory_space=pl.ANY)
    drift_shape = jax.ShapeDtypeStruct((height, breadth), jnp.float32)
    low = jnp.bfloat16
    rows_shape = (nc, height, breadth)
    cols_shape = (nz, height, breadth)
    wide_shape = jax.ShapeDtypeStruct((height + 2 * OMAX, breadth + 2 * LANES), low)
    out_shape = [drift_shape, drift_shape, wide_shape, wide_shape]
    out_specs = [vmem] * 4
    if first:
        out_shape += [jax.ShapeDtypeStruct(rows_shape, low), jax.ShapeDtypeStruct(cols_shape, low)]
        out_specs += [anywhere, anywhere]
        in_specs = [vmem] * 3
        operands = (real_low, imag_low, ham)
    else:
        in_specs = [vmem, vmem, anywhere, anywhere]
        operands = (real_low, imag_low) + tuple(panels)
    count = 4 if first else 2
    flops = 8 * height * breadth * nz * height
    return pl.pallas_call(
        functools.partial(commutator_kernel, first, nz, nc),
        out_shape=out_shape,
        in_specs=in_specs,
        out_specs=out_specs,
        scratch_shapes=[
            pltpu.VMEM(rows_shape, low),
            pltpu.VMEM(cols_shape, low),
            pltpu.VMEM(rows_shape, low),
            pltpu.VMEM(rows_shape, low),
            pltpu.VMEM(cols_shape, low),
            pltpu.VMEM(cols_shape, low),
            pltpu.VMEM((8, OMAX, LANES), low),
            pltpu.SemaphoreType.DMA((count, nc)),
            pltpu.SemaphoreType.DMA((count, nc)),
            pltpu.SemaphoreType.DMA((count, 2, nz)),
            pltpu.SemaphoreType.DMA((count, 2, nz)),
            pltpu.SemaphoreType.DMA((8,)),
            pltpu.SemaphoreType.DMA((8,)),
            pltpu.SemaphoreType.DMA((2,)),
        ],
        compiler_params=pltpu.CompilerParams(
            collective_id=0 if first else 1, has_side_effects=True, vmem_limit_bytes=VMEM_LIMIT
        ),
        cost_estimate=pl.CostEstimate(flops=flops, bytes_accessed=16 * height * breadth, transcendentals=0),
        name="first_commutator" if first else "second_commutator",
    )(*operands)


def diagonal_sum(matrix, row_first, col_first):
    row_index = lax.broadcasted_iota(jnp.int32, matrix.shape, 0) + row_first
    col_index = lax.broadcasted_iota(jnp.int32, matrix.shape, 1) + col_first
    return jnp.sum(jnp.where(row_index == col_index, matrix, 0.0))


def dissipate_kernel(last, slots, offsets, scale, *refs):
    if last:
        (real, imag, first_real, first_imag, turn_real, turn_imag, real_wide, imag_wide,
         row_rate, col_rate, out_real, out_imag, real_full, imag_full) = refs
    else:
        (real, imag, turn_real, turn_imag, real_wide, imag_wide,
         row_rate, col_rate, out_real, out_imag, low_real, low_imag, real_full, imag_full) = refs
    step = pl.program_id(0)
    tile, breadth = real.shape
    width = real_full.shape[1]
    factor = scale[0]

    @pl.when(step == 0)
    def _():
        rows = pl.ds(0, real_wide.shape[0])
        real_full[rows, :] = real_wide[...].astype(jnp.float32)
        imag_full[rows, :] = imag_wide[...].astype(jnp.float32)

    sums = [jnp.zeros((tile, breadth), jnp.float32) for _ in range(2)]
    for slot in range(slots):
        offset = offsets[slot]
        whole_rows = (OMAX + offset) // 8
        spare_rows = OMAX + offset - whole_rows * 8
        weight = row_rate[:, slot : slot + 1] * col_rate[slot : slot + 1, :]
        for side, full in enumerate((real_full, imag_full)):
            strip = full[pl.ds(pl.multiple_of(step * tile + whole_rows * 8, 8), tile + 8), :]
            strip = pltpu.roll(strip, width - LANES - offset, 1)[:, :breadth]
            strip = pltpu.roll(strip, lax.rem(tile + 8 - spare_rows, tile + 8), 0)[:tile, :]
            sums[side] += weight * strip
    loss = -0.5 * (row_rate[:, slots : slots + 1] + col_rate[slots : slots + 1, :])
    if last:
        sides = ((real, first_real, turn_real, out_real), (imag, first_imag, turn_imag, out_imag))
        for side, (start, first, turn, out) in enumerate(sides):
            middle = (start[...] + step_size * first[...]) * factor
            second = turn[...] + sums[side] + loss * middle
            out[...] = (start[...] + 0.5 * step_size * (first[...] + second)) * factor
    else:
        sides = ((real, turn_real, out_real, low_real), (imag, turn_imag, out_imag, low_imag))
        for side, (start, turn, out, low) in enumerate(sides):
            first = turn[...] + sums[side] + loss * start[...]
            out[...] = first
            low[...] = ((start[...] + step_size * first) * factor).astype(jnp.bfloat16)


def finish_drift(last, offsets, scale, tiled, wides, row_rate, col_rate):
    height, breadth = tiled[0].shape
    slots = offsets.shape[0]
    tile = min(128, height)
    smem = pl.BlockSpec(memory_space=pltpu.SMEM)
    block = pl.BlockSpec((tile, breadth), lambda i: (i, 0))

    def whole(array):
        return pl.BlockSpec(array.shape, lambda i: (0, 0))

    shape = jax.ShapeDtypeStruct((height, breadth), jnp.float32)
    low_shape = jax.ShapeDtypeStruct((height, breadth), jnp.bfloat16)
    out_shape = [shape, shape] if last else [shape, shape, low_shape, low_shape]
    return pl.pallas_call(
        functools.partial(dissipate_kernel, last, slots),
        grid=(height // tile,),
        out_shape=out_shape,
        in_specs=[smem, smem]
        + [block] * len(tiled)
        + [whole(wide) for wide in wides]
        + [pl.BlockSpec((tile, row_rate.shape[1]), lambda i: (i, 0)), whole(col_rate)],
        out_specs=[block] * len(out_shape),
        scratch_shapes=[pltpu.VMEM((wides[0].shape[0] + 8, wides[0].shape[1]), jnp.float32)] * 2,
        compiler_params=pltpu.CompilerParams(
            dimension_semantics=("arbitrary",), vmem_limit_bytes=40 * 1024 * 1024
        ),
        cost_estimate=pl.CostEstimate(
            flops=60 * height * breadth, bytes_accessed=40 * height * breadth, transcendentals=0
        ),
        name="last_dissipator" if last else "first_dissipator",
    )(offsets, scale, *tiled, *wides, row_rate, col_rate)


def rates(amplitudes, offsets, active):
    slots, levels = amplitudes.shape
    positions = jnp.arange(levels, dtype=jnp.int32)
    target = positions[None, :] + offsets[:, None]
    inside = (target >= 0) & (target < levels) & (jnp.arange(slots)[:, None] < active)
    strength = jnp.where(inside, amplitudes, 0.0)
    squares = jnp.pad(strength * strength, ((0, 0), (OMAX, OMAX)))
    outflow = jnp.zeros((levels,), jnp.float32)
    for slot in range(slots):
        outflow = outflow + lax.dynamic_slice(squares, (slot, OMAX - offsets[slot]), (1, levels))[0]
    return jnp.concatenate([strength, outflow[None, :], jnp.zeros((7, levels), jnp.float32)], axis=0)


def local(nz, nc, rho_real, rho_imag, hamiltonian, amplitudes, offsets, active_jumps):
    height, breadth = rho_real.shape
    levels = amplitudes.shape[1]
    row_first = lax.axis_index("row") * height
    col_first = lax.axis_index("col") * breadth
    partial = diagonal_sum(rho_real, row_first, col_first)
    partials = lax.all_gather(jnp.full((8, LANES), partial), ("row", "col"), axis=0, tiled=False)
    scale = (levels / jnp.sum(partials[:, 0, 0])).reshape(1)
    table = rates(amplitudes, offsets, active_jumps[0])
    row_rate = lax.dynamic_slice_in_dim(table, row_first, height, axis=1).T
    col_rate = lax.dynamic_slice_in_dim(table, col_first, breadth, axis=1)

    turn_real, turn_imag, real_wide, imag_wide, *panels = commutator(
        rho_real.astype(jnp.bfloat16), rho_imag.astype(jnp.bfloat16), hamiltonian, None, nz, nc
    )
    first_real, first_imag, low_real, low_imag = finish_drift(
        False, offsets, scale, (rho_real, rho_imag, turn_real, turn_imag), (real_wide, imag_wide), row_rate, col_rate
    )
    turn_real, turn_imag, real_wide, imag_wide = commutator(low_real, low_imag, hamiltonian, panels, nz, nc)
    return tuple(
        finish_drift(
            True,
            offsets,
            scale,
            (rho_real, rho_imag, first_real, first_imag, turn_real, turn_imag),
            (real_wide, imag_wide),
            row_rate,
            col_rate,
        )
    )


def solution(mesh):
    in_specs = (P("row", "col"), P("row", "col"), P("row", "col"), P(), P(), P())
    out_specs = (P("row", "col"), P("row", "col"))
    body = functools.partial(local, mesh.shape["row"], mesh.shape["col"])
    return jax.shard_map(body, mesh=mesh, in_specs=in_specs, out_specs=out_specs, check_vma=False)
```

```python
import functools

import jax
import jax.numpy as jnp
from jax import lax
from jax.experimental import pallas as pl
from jax.experimental.pallas import tpu as pltpu
from jax.sharding import PartitionSpec as P

OMAX = 16
LANES = 128


step_size = 0.25

VMEM_LIMIT = 62 * 1024 * 1024


def ring_plan(count, favour_up):
    far = count // 2
    near = count - 1 - far
    return (far, near) if favour_up else (near, far)


def top(mask):
    return mask.bit_length() - 1


def commutator_kernel(first, nz, nc, *refs):
    if first:
        (real, imag, ham, out_real, out_imag, real_wide, imag_wide, ham_rows_out, ham_cols_out,
         ham_rows, ham_cols, real_rows, imag_rows, real_cols, imag_cols, corners,
         xy_send, xy_recv, z_send, z_recv, corner_send, corner_recv, local_sem) = refs
    else:
        (real, imag, ham_rows_in, ham_cols_in, out_real, out_imag, real_wide, imag_wide,
         ham_rows, ham_cols, real_rows, imag_rows, real_cols, imag_cols, corners,
         xy_send, xy_recv, z_send, z_recv, corner_send, corner_recv, local_sem) = refs
        ham = None
    height, breadth = real.shape
    z = lax.axis_index("row")
    c = lax.axis_index("col")
    bits = nc.bit_length() - 1
    half = height // 2
    physical = list(range(1, bits))
    order_a = physical + [0]
    order_b = physical[::-1] + [0]

    pieces = []
    if first:
        pieces.append((ham, ham_rows, (0, half), order_a))
        pieces.append((ham, ham_rows, (half, half), order_b))
    pieces.append((real, real_rows, (0, height), order_a))
    pieces.append((imag, imag_rows, (0, height), order_b))
    rings = []
    if first:
        rings.append((ham, ham_cols, (0, half), True))
        rings.append((ham, ham_cols, (half, half), False))
    rings.append((real, real_cols, (0, height), True))
    rings.append((imag, imag_cols, (0, height), False))

    barrier = pltpu.get_barrier_semaphore()
    up = lax.rem(z + 1, nz)
    down = lax.rem(z + nz - 1, nz)

    def flip(index, b):
        weight = 1 << b
        bit = lax.rem(index // weight, 2)
        return index + weight * (1 - 2 * bit)

    def masked(mask, order):
        index = c
        for t in range(bits):
            if mask >> t & 1:
                index = flip(index, order[t])
        return index

    for neighbour in (up, down):
        pl.semaphore_signal(barrier, inc=1, device_id=(neighbour, c), device_id_type=pl.DeviceIdType.MESH)
    for b in range(bits):
        pl.semaphore_signal(barrier, inc=1, device_id=(z, flip(c, b)), device_id_type=pl.DeviceIdType.MESH)
    left = lax.rem(c + nc - 1, nc)
    right = lax.rem(c + 1, nc)
    diagonals = [(v, h) for v in (0, 1) for h in (0, 1)]

    def diagonal(v, h):
        return ((up, down)[v], (right, left)[h])

    for v, h in diagonals:
        pl.semaphore_signal(barrier, inc=1, device_id=diagonal(v, h), device_id_type=pl.DeviceIdType.MESH)
    pl.semaphore_wait(barrier, 2 + bits + 4)

    def corner_copy(side, v, h):
        own = (real, imag)[side]
        rows = pl.ds(height - OMAX if v == 0 else 0, OMAX)
        cols = pl.ds(breadth - LANES if h == 0 else 0, LANES)
        slot = side * 4 + v * 2 + h
        return pltpu.make_async_remote_copy(
            src_ref=own.at[rows, cols],
            dst_ref=corners.at[slot],
            send_sem=corner_send.at[slot],
            recv_sem=corner_recv.at[slot],
            device_id=diagonal(v, h),
            device_id_type=pl.DeviceIdType.MESH,
        )

    def xy_copy(p, mask, t):
        own, panel, (start, size), order = pieces[p]
        index = masked(mask, order)
        rows = pl.ds(start, size)
        source = own.at[rows, :] if mask == 0 else panel.at[index, rows, :]
        arrival = mask | 1 << t
        return pltpu.make_async_remote_copy(
            src_ref=source,
            dst_ref=panel.at[index, rows, :],
            send_sem=xy_send.at[p, arrival],
            recv_sem=xy_recv.at[p, arrival],
            device_id=(z, flip(c, order[t])),
            device_id_type=pl.DeviceIdType.MESH,
        )

    def z_copy(p, direction, step):
        own, panel, (start, size), _ = rings[p]
        rows = pl.ds(start, size)
        shift = nz - (step - 1) if direction == 0 else step - 1
        index = lax.rem(z + shift, nz)
        source = own.at[rows, :] if step == 1 else panel.at[index, rows, :]
        return pltpu.make_async_remote_copy(
            src_ref=source,
            dst_ref=panel.at[index, rows, :],
            send_sem=z_send.at[p, direction, step],
            recv_sem=z_recv.at[p, direction, step],
            device_id=(up if direction == 0 else down, c),
            device_id_type=pl.DeviceIdType.MESH,
        )

    started = []

    def begin(copy):
        copy.start()
        started.append(copy)

    def begin_own(which):
        for p in which:
            for t in range(bits):
                begin(xy_copy(p, 0, t))
            plan = ring_plan(nz, rings[p][3])
            for direction in (0, 1):
                if plan[direction] >= 1:
                    begin(z_copy(p, direction, 1))

    for side in (0, 1):
        for v, h in diagonals:
            begin(corner_copy(side, v, h))
    begin_own((0, 1))

    if first:
        locals_in = [
            pltpu.make_async_copy(ham, ham_rows.at[c], local_sem.at[0]),
            pltpu.make_async_copy(ham, ham_cols.at[z], local_sem.at[1]),
        ]
    else:
        locals_in = [
            pltpu.make_async_copy(ham_rows_in, ham_rows, local_sem.at[0]),
            pltpu.make_async_copy(ham_cols_in, ham_cols, local_sem.at[1]),
        ]
    for copy in locals_in:
        copy.start()

    def advance_xy(p, mask):
        order_t = top(mask)
        xy_copy(p, mask & ~(1 << order_t), order_t).wait_recv()
        for t in range(order_t + 1, bits):
            begin(xy_copy(p, mask, t))

    def advance_z(p, direction, step):
        plan = ring_plan(nz, rings[p][3])
        z_copy(p, direction, step).wait_recv()
        if step < plan[direction]:
            begin(z_copy(p, direction, step + 1))

    ring_steps = max(ring_plan(nz, True))

    def ring_events(p, step):
        plan = ring_plan(nz, rings[p][3])
        return [(p, d, step) for d in (0, 1) if step <= plan[d]]

    base = 0
    if first:
        base = 2
        for mask in range(1, nc):
            for p in (0, 1):
                advance_xy(p, mask)
            if mask <= ring_steps:
                for p in (0, 1):
                    for event in ring_events(p, mask):
                        advance_z(*event)
            if mask == 1:
                begin_own((2, 3))
        for step in range(nc, ring_steps + 1):
            for p in (0, 1):
                for event in ring_events(p, step):
                    advance_z(*event)
    for copy in locals_in:
        copy.wait()
    outs = []
    if first:
        outs = [
            pltpu.make_async_copy(ham_rows, ham_rows_out, local_sem.at[0]),
            pltpu.make_async_copy(ham_cols, ham_cols_out, local_sem.at[1]),
        ]
        for copy in outs:
            copy.start()

    per = height // breadth
    tile = min(256, height)

    def rows_product(out, block, index, sign, fresh):
        k = index // per
        offset = pl.multiple_of(lax.rem(index, per) * breadth, breadth)

        @pl.loop(0, height // tile)
        def _(i):
            here = pl.ds(pl.multiple_of(i * tile, tile), tile)
            product = jnp.dot(
                block[here, :], ham_cols[k, pl.ds(offset, breadth), :], preferred_element_type=jnp.float32
            )
            if fresh:
                out[here, :] = product if sign > 0 else -product
            elif sign > 0:
                out[here, :] += product
            else:
                out[here, :] -= product

    def cols_product(out, block, k, sign):
        @pl.loop(0, height // tile)
        def _(i):
            here = pl.ds(pl.multiple_of(i * tile, tile), tile)
            product = jnp.dot(
                ham_rows[k * per, here, :], block[pl.ds(0, breadth), :], preferred_element_type=jnp.float32
            )
            for part in range(1, per):
                product += jnp.dot(
                    ham_rows[k * per + part, here, :],
                    block[pl.ds(part * breadth, breadth), :],
                    preferred_element_type=jnp.float32,
                )
            if sign > 0:
                out[here, :] += product
            else:
                out[here, :] -= product

    rows_product(out_imag, real, c, 1, True)
    rows_product(out_real, imag, c, -1, True)
    cols_product(out_imag, real, z, -1)
    cols_product(out_real, imag, z, 1)
    sides = ((real_rows, real_cols, out_imag, 1), (imag_rows, imag_cols, out_real, -1))

    def consume_ring(step):
        for side, (_, cols, out, sign) in enumerate(sides):
            for p, direction, s in ring_events(base + side, step):
                advance_z(p, direction, s)
                shift = nz - s if direction == 0 else s
                k = lax.rem(z + shift, nz)
                cols_product(out, cols.at[k], k, -sign)

    done_steps = 0
    for mask in range(1, nc):
        for side, (rows, _, out, sign) in enumerate(sides):
            p = base + side
            advance_xy(p, mask)
        for side, (rows, _, out, sign) in enumerate(sides):
            index = masked(mask, pieces[base + side][3])
            rows_product(out, rows.at[index], index, sign, False)
        want = mask * ring_steps // (nc - 1) if nc > 1 else ring_steps
        while done_steps < want:
            done_steps += 1
            consume_ring(done_steps)
    for side, (rows, cols, wide) in enumerate(((real_rows, real_cols, real_wide), (imag_rows, imag_cols, imag_wide))):
        own = (real, imag)[side]
        for v, h in diagonals:
            corner_copy(side, v, h).wait_recv()
        middle = pl.ds(OMAX, height)
        inner = pl.ds(LANES, breadth)
        above, below = pl.ds(0, OMAX), pl.ds(OMAX + height, OMAX)
        before, after = pl.ds(0, LANES), pl.ds(LANES + breadth, LANES)
        wide[middle, inner] = own[...]
        wide[above, inner] = cols[down, pl.ds(height - OMAX, OMAX), :]
        wide[below, inner] = cols[up, pl.ds(0, OMAX), :]
        wide[middle, before] = rows[left, :, pl.ds(breadth - LANES, LANES)]
        wide[middle, after] = rows[right, :, pl.ds(0, LANES)]
        wide[above, before] = corners[side * 4]
        wide[above, after] = corners[side * 4 + 1]
        wide[below, before] = corners[side * 4 + 2]
        wide[below, after] = corners[side * 4 + 3]
    for copy in started:
        copy.wait_send()
    for copy in outs:
        copy.wait()


def commutator(real_low, imag_low, ham, panels, nz, nc):
    height, breadth = real_low.shape
    first = panels is None
    vmem = pl.BlockSpec(memory_space=pltpu.VMEM)
    anywhere = pl.BlockSpec(memory_space=pl.ANY)
    drift_shape = jax.ShapeDtypeStruct((height, breadth), jnp.float32)
    low = jnp.bfloat16
    rows_shape = (nc, height, breadth)
    cols_shape = (nz, height, breadth)
    wide_shape = jax.ShapeDtypeStruct((height + 2 * OMAX, breadth + 2 * LANES), low)
    out_shape = [drift_shape, drift_shape, wide_shape, wide_shape]
    out_specs = [vmem] * 4
    if first:
        out_shape += [jax.ShapeDtypeStruct(rows_shape, low), jax.ShapeDtypeStruct(cols_shape, low)]
        out_specs += [anywhere, anywhere]
        in_specs = [vmem] * 3
        operands = (real_low, imag_low, ham)
    else:
        in_specs = [vmem, vmem, anywhere, anywhere]
        operands = (real_low, imag_low) + tuple(panels)
    count = 4 if first else 2
    flops = 8 * height * breadth * nz * height
    return pl.pallas_call(
        functools.partial(commutator_kernel, first, nz, nc),
        out_shape=out_shape,
        in_specs=in_specs,
        out_specs=out_specs,
        scratch_shapes=[
            pltpu.VMEM(rows_shape, low),
            pltpu.VMEM(cols_shape, low),
            pltpu.VMEM(rows_shape, low),
            pltpu.VMEM(rows_shape, low),
            pltpu.VMEM(cols_shape, low),
            pltpu.VMEM(cols_shape, low),
            pltpu.VMEM((8, OMAX, LANES), low),
            pltpu.SemaphoreType.DMA((count, nc)),
            pltpu.SemaphoreType.DMA((count, nc)),
            pltpu.SemaphoreType.DMA((count, 2, nz)),
            pltpu.SemaphoreType.DMA((count, 2, nz)),
            pltpu.SemaphoreType.DMA((8,)),
            pltpu.SemaphoreType.DMA((8,)),
            pltpu.SemaphoreType.DMA((2,)),
        ],
        compiler_params=pltpu.CompilerParams(
            collective_id=0 if first else 1, has_side_effects=True, vmem_limit_bytes=VMEM_LIMIT
        ),
        cost_estimate=pl.CostEstimate(flops=flops, bytes_accessed=16 * height * breadth, transcendentals=0),
        name="first_commutator" if first else "second_commutator",
    )(*operands)


def diagonal_sum(matrix, row_first, col_first):
    row_index = lax.broadcasted_iota(jnp.int32, matrix.shape, 0) + row_first
    col_index = lax.broadcasted_iota(jnp.int32, matrix.shape, 1) + col_first
    return jnp.sum(jnp.where(row_index == col_index, matrix, 0.0))


def dissipate_kernel(last, slots, offsets, scale, *refs):
    if last:
        (real, imag, first_real, first_imag, turn_real, turn_imag, real_wide, imag_wide,
         row_rate, col_rate, out_real, out_imag, real_full, imag_full) = refs
    else:
        (real, imag, turn_real, turn_imag, real_wide, imag_wide,
         row_rate, col_rate, out_real, out_imag, low_real, low_imag, real_full, imag_full) = refs
    step = pl.program_id(0)
    tile, breadth = real.shape
    width = real_full.shape[1]
    factor = scale[0]

    @pl.when(step == 0)
    def _():
        rows = pl.ds(0, real_wide.shape[0])
        real_full[rows, :] = real_wide[...].astype(jnp.float32)
        imag_full[rows, :] = imag_wide[...].astype(jnp.float32)

    sums = [jnp.zeros((tile, breadth), jnp.float32) for _ in range(2)]
    for slot in range(slots):
        offset = offsets[slot]
        whole_rows = (OMAX + offset) // 8
        spare_rows = OMAX + offset - whole_rows * 8
        weight = row_rate[:, slot : slot + 1] * col_rate[slot : slot + 1, :]
        for side, full in enumerate((real_full, imag_full)):
            strip = full[pl.ds(pl.multiple_of(step * tile + whole_rows * 8, 8), tile + 8), :]
            strip = pltpu.roll(strip, width - LANES - offset, 1)[:, :breadth]
            strip = pltpu.roll(strip, lax.rem(tile + 8 - spare_rows, tile + 8), 0)[:tile, :]
            sums[side] += weight * strip
    loss = -0.5 * (row_rate[:, slots : slots + 1] + col_rate[slots : slots + 1, :])
    if last:
        sides = ((real, first_real, turn_real, out_real), (imag, first_imag, turn_imag, out_imag))
        for side, (start, first, turn, out) in enumerate(sides):
            middle = (start[...] + step_size * first[...]) * factor
            second = turn[...] + sums[side] + loss * middle
            out[...] = (start[...] + 0.5 * step_size * (first[...] + second)) * factor
    else:
        sides = ((real, turn_real, out_real, low_real), (imag, turn_imag, out_imag, low_imag))
        for side, (start, turn, out, low) in enumerate(sides):
            first = turn[...] + sums[side] + loss * start[...]
            out[...] = first
            low[...] = ((start[...] + step_size * first) * factor).astype(jnp.bfloat16)


def finish_drift(last, offsets, scale, tiled, wides, row_rate, col_rate):
    height, breadth = tiled[0].shape
    slots = offsets.shape[0]
    tile = min(128, height)
    smem = pl.BlockSpec(memory_space=pltpu.SMEM)
    block = pl.BlockSpec((tile, breadth), lambda i: (i, 0))

    def whole(array):
        return pl.BlockSpec(array.shape, lambda i: (0, 0))

    shape = jax.ShapeDtypeStruct((height, breadth), jnp.float32)
    low_shape = jax.ShapeDtypeStruct((height, breadth), jnp.bfloat16)
    out_shape = [shape, shape] if last else [shape, shape, low_shape, low_shape]
    return pl.pallas_call(
        functools.partial(dissipate_kernel, last, slots),
        grid=(height // tile,),
        out_shape=out_shape,
        in_specs=[smem, smem]
        + [block] * len(tiled)
        + [whole(wide) for wide in wides]
        + [pl.BlockSpec((tile, row_rate.shape[1]), lambda i: (i, 0)), whole(col_rate)],
        out_specs=[block] * len(out_shape),
        scratch_shapes=[pltpu.VMEM((wides[0].shape[0] + 8, wides[0].shape[1]), jnp.float32)] * 2,
        compiler_params=pltpu.CompilerParams(
            dimension_semantics=("arbitrary",), vmem_limit_bytes=VMEM_LIMIT
        ),
        cost_estimate=pl.CostEstimate(
            flops=60 * height * breadth, bytes_accessed=40 * height * breadth, transcendentals=0
        ),
        name="last_dissipator" if last else "first_dissipator",
    )(offsets, scale, *tiled, *wides, row_rate, col_rate)


def rates(amplitudes, offsets, active):
    slots, levels = amplitudes.shape
    positions = jnp.arange(levels, dtype=jnp.int32)
    target = positions[None, :] + offsets[:, None]
    inside = (target >= 0) & (target < levels) & (jnp.arange(slots)[:, None] < active)
    strength = jnp.where(inside, amplitudes, 0.0)
    squares = jnp.pad(strength * strength, ((0, 0), (OMAX, OMAX)))
    outflow = jnp.zeros((levels,), jnp.float32)
    for slot in range(slots):
        outflow = outflow + lax.dynamic_slice(squares, (slot, OMAX - offsets[slot]), (1, levels))[0]
    return jnp.concatenate([strength, outflow[None, :], jnp.zeros((7, levels), jnp.float32)], axis=0)


def local(nz, nc, rho_real, rho_imag, hamiltonian, amplitudes, offsets, active_jumps):
    height, breadth = rho_real.shape
    levels = amplitudes.shape[1]
    row_first = lax.axis_index("row") * height
    col_first = lax.axis_index("col") * breadth
    partial = diagonal_sum(rho_real, row_first, col_first)
    start_trace = lax.psum(lax.psum(partial, "row"), "col")
    scale = (levels / start_trace).reshape(1)
    table = rates(amplitudes, offsets, active_jumps[0])
    row_rate = lax.dynamic_slice_in_dim(table, row_first, height, axis=1).T
    col_rate = lax.dynamic_slice_in_dim(table, col_first, breadth, axis=1)

    turn_real, turn_imag, real_wide, imag_wide, *panels = commutator(
        rho_real.astype(jnp.bfloat16), rho_imag.astype(jnp.bfloat16), hamiltonian, None, nz, nc
    )
    first_real, first_imag, low_real, low_imag = finish_drift(
        False, offsets, scale, (rho_real, rho_imag, turn_real, turn_imag), (real_wide, imag_wide), row_rate, col_rate
    )
    turn_real, turn_imag, real_wide, imag_wide = commutator(low_real, low_imag, hamiltonian, panels, nz, nc)
    return tuple(
        finish_drift(
            True,
            offsets,
            scale,
            (rho_real, rho_imag, first_real, first_imag, turn_real, turn_imag),
            (real_wide, imag_wide),
            row_rate,
            col_rate,
        )
    )


def solution(mesh):
    in_specs = (P("row", "col"), P("row", "col"), P("row", "col"), P(), P(), P())
    out_specs = (P("row", "col"), P("row", "col"))
    body = functools.partial(local, mesh.shape["row"], mesh.shape["col"])
    return jax.shard_map(body, mesh=mesh, in_specs=in_specs, out_specs=out_specs, check_vma=False)
```
